128 devices in a mesh: gx: 16 (over y, z_hi, core), gy: 8 (over z_lo, x).
Axes of the slice: x: 4, y: 4, z: 4 (z_hi: 2, z_lo: 2; z = z_hi * 2 + z_lo), core: 2. Of those that a mesh axis runs over, the one named last changes fastest.
Arguments:
- subspace: float32 [65536, 256], P(('gx', 'gy')), may hold values from -15 to 15
- diag_blocks: float32 [128, 512, 512], P(('gx', 'gy')), may hold values from -0.25 to 0.25
- onsite: float32 [65536], P(('gx', 'gy')), may hold values from 0.5 to 4
- coupling: float32 [2, 128, 12, 128, 128], P(None, ('gx', 'gy')), may hold values from -0.1875 to 0.1875
- tile_rows: int32 [2, 128, 12], P(None, ('gx', 'gy')), may hold values from 0 to 3
- tile_cols: int32 [2, 128, 12], P(None, ('gx', 'gy')), may hold values from 0 to 3
- partner: int32 [2, 128], replicated, may hold values from 0 to 127, as said below
Outputs:
- basis: float32 [65536, 256], P(('gx', 'gy'))
- gram_scaled: float32 [256, 256], replicated
The draws below stay inside these ranges and needn't reach their ends.
Inputs may be any that keep to these rules, and one draw needn't show every extreme that they name: For each colour c there is one m_c, 1 to 127, with partner[c, i] = i XOR m_c for every device i; the two colours' m differ.
All inputs are finite; a program needn't handle non-finite values.
Results may differ from the reference program's by a relative error of at most 0.0003.
Values sent between devices are 32-bit elements; how exact they have to be, the bound alone decides.
No kernel may reach another device: no remote copies, remote signals or barrier semaphores. Data moves between devices by JAX's collectives and lax.ppermute only.
A program may use at most 64 MiB of HBM per device.

```python
import math
import jax
import jax.numpy as jnp
from jax import lax

STATES = 256
TILE = 128
ROWS_DEV = 512
TILES = 12
COLOURS = 2
NS_ITERS = 12
BLOCKS = 4
NROWS = 65536
N_GX = 16
N_GY = 8


def draw_partner(key, part):
    devices = N_GX * N_GY
    lead_key, tail_key = jax.random.split(jax.random.fold_in(key, 11))
    lead_mask = jax.random.randint(lead_key, (), 1, devices, dtype=jnp.int32)
    offset = jax.random.randint(tail_key, (), 1, devices - 1, dtype=jnp.int32)
    tail_mask = (lead_mask - 1 + offset) % (devices - 1) + 1
    partner_masks = jnp.stack([lead_mask, tail_mask]).astype(jnp.int32)
    device_ids = jnp.arange(devices, dtype=jnp.int32)
    return jnp.bitwise_xor(device_ids[None, :], partner_masks[:, None]).astype(jnp.int32)


def draw_subspace(key, part):
    column_key, base_key = jax.random.split(jax.random.fold_in(key, 23), 2)
    column_scale = jnp.exp(jax.random.uniform(column_key, (STATES,), jnp.float32, math.log(0.3), math.log(3.0)))
    base = jnp.clip(jax.random.normal(base_key, (NROWS, STATES), jnp.float32), -5.0, 5.0)
    return (base * column_scale[None, :]).astype(jnp.float32)


def plant(values, own_key, low, largest):
    shape = values.shape
    place = [jax.random.randint(jax.random.fold_in(own_key, axis), (), 0, shape[axis]) for axis in range(len(shape))]
    values = values.at[tuple(place)].set(low)
    longest = shape.index(max(shape))
    place[longest] = (place[longest] + 1) % shape[longest]
    return values.at[tuple(place)].set(largest)


def block_scale(own_key, extent, shards, low, high):
    level = 1.0
    for position, parts in shards:
        heights = jax.random.uniform(jax.random.fold_in(jax.random.fold_in(own_key, 6), position), (parts,), jnp.float32, low / len(shards), high / len(shards))
        level = level * jnp.repeat(jnp.exp(heights), extent[position] // parts).reshape((-1,) + (1,) * (len(extent) - 1 - position))
    return level


def centred(stream_key, dims, scale, most, cuts=(), kind=jnp.bfloat16):
    values = scale * jax.random.normal(stream_key, dims, jnp.float32)
    if cuts:
        values = values * block_scale(stream_key, dims, cuts, -0.22, 0.18)
    return jnp.clip(values, -most, most).astype(kind)


def setup_inputs(seed: int = 0) -> dict:
    seeds = jax.random.split(jax.random.key(seed), 8)
    subspace = draw_subspace(jax.random.fold_in(seeds[7], 71), 0)
    diag_blocks = centred(seeds[1], (N_GX * N_GY, ROWS_DEV, ROWS_DEV), ROWS_DEV ** -0.5, 0.25, ((0, 128),), jnp.float32)
    onsite = jnp.clip(jnp.exp(math.log(4.0) - 2.0794415 * jax.random.uniform(seeds[2], (NROWS,), jnp.float32) ** block_scale(seeds[2], (NROWS,), ((0, 128),), -0.2, 0.2)), 0.5, 4.0)
    coupling = centred(seeds[3], (COLOURS, N_GX * N_GY, TILES, TILE, TILE), (TILE * 8) ** -0.5, 0.1875, ((1, 128),), jnp.float32)
    tile_rows = plant(jax.random.randint(seeds[4], (COLOURS, N_GX * N_GY, TILES), 0, BLOCKS), jax.random.fold_in(seeds[4], 1), 0, BLOCKS - 1).astype(jnp.int32)
    tile_cols = plant(jax.random.randint(seeds[5], (COLOURS, N_GX * N_GY, TILES), 0, BLOCKS), jax.random.fold_in(seeds[5], 1), 0, BLOCKS - 1).astype(jnp.int32)
    partner = draw_partner(jax.random.fold_in(seeds[7], 71), 0)
    return dict(subspace=subspace, diag_blocks=diag_blocks, onsite=onsite, coupling=coupling, tile_rows=tile_rows, tile_cols=tile_cols, partner=partner)


def apply_tiles(coupling_part, targets, picks, source, transposed):
    picked = source[picks]
    if transposed:
        products = jnp.einsum('kji,kjm->kim', coupling_part, picked, precision=lax.Precision.HIGHEST)
    else:
        products = jnp.einsum('kij,kjm->kim', coupling_part, picked, precision=lax.Precision.HIGHEST)
    placing = (targets[None, :] == jnp.arange(source.shape[0], dtype=jnp.int32)[:, None]).astype(jnp.float32)
    return jnp.einsum('bk,kim->bim', placing, products, precision=lax.Precision.HIGHEST)

def apply_hamiltonian(vectors, diag_blocks, onsite, coupling, tile_rows, tile_cols, partner):
    devices = N_GX * N_GY
    all_blocks = vectors.reshape(devices, BLOCKS, TILE, STATES)
    onsite_rows = onsite.reshape(devices, ROWS_DEV)

    def one_device(index):
        own_flat = all_blocks[index].reshape(ROWS_DEV, STATES)
        result = jnp.dot(diag_blocks[index], own_flat, precision=lax.Precision.HIGHEST, preferred_element_type=jnp.float32)
        result = result + onsite_rows[index][:, None] * own_flat
        for colour in range(COLOURS):
            mate = partner[colour, index]
            source = all_blocks[mate]
            forward = apply_tiles(coupling[colour, index], tile_rows[colour, index], tile_cols[colour, index], source, False)
            backward = apply_tiles(coupling[colour, mate], tile_cols[colour, mate], tile_rows[colour, mate], source, True)
            result = result + (forward + backward).reshape(ROWS_DEV, STATES)
        return result
    return lax.map(one_device, jnp.arange(devices, dtype=jnp.int32)).reshape(devices * ROWS_DEV, STATES)

def reference(subspace, diag_blocks, onsite, coupling, tile_rows, tile_cols, partner):

    def hamiltonian(vectors):
        return apply_hamiltonian(vectors, diag_blocks, onsite, coupling, tile_rows, tile_cols, partner)
    first = (hamiltonian(subspace) - 2.0 * subspace) / 4.0
    filtered = (hamiltonian(first) - 2.0 * first) / 2.0 - subspace
    gram_sum = jnp.dot(filtered.T, filtered, precision=lax.Precision.HIGHEST, preferred_element_type=jnp.float32)
    total_diag = jnp.trace(gram_sum)
    identity = jnp.eye(STATES, dtype=jnp.float32)
    iterate = gram_sum / total_diag
    inverse = identity
    for turn_index in range(NS_ITERS):
        factor = 1.5 * identity - 0.5 * jnp.dot(inverse, iterate, precision=lax.Precision.HIGHEST)
        iterate, inverse = (jnp.dot(iterate, factor, precision=lax.Precision.HIGHEST), jnp.dot(factor, inverse, precision=lax.Precision.HIGHEST))
    basis = jnp.dot(filtered, inverse, precision=lax.Precision.HIGHEST) * (jnp.sqrt(jnp.float32(NROWS)) / jnp.sqrt(total_diag))
    return (basis, gram_sum / NROWS)
```

```python
import functools

import jax
import jax.numpy as jnp
from jax import lax
from jax.experimental import pallas as pl
from jax.experimental.pallas import tpu as pltpu
from jax.sharding import PartitionSpec as P

NS_ITERS = 12
AXES = ("gx", "gy")
VMEM = pl.BlockSpec(memory_space=pltpu.VMEM)
SMEM = pl.BlockSpec(memory_space=pltpu.SMEM)
F32 = jnp.float32
BF16 = jnp.bfloat16
LANES = 128
NN = (((1,), (0,)), ((), ()))
TN = (((0,), (0,)), ((), ()))


def devices():
    return lax.axis_size("gx") * lax.axis_size("gy")


def swap(value, flip):
    return lax.ppermute(value, AXES, [(i, i ^ flip) for i in range(devices())])


def exchange(mask, value):
    branches = [functools.partial(swap, flip=flip) for flip in range(1, devices())]
    return lax.switch(mask - 1, branches, value)


def split(value):
    high = value.astype(BF16)
    return high, (value - high.astype(F32)).astype(BF16)


def product(left, right, dims=NN):
    dot = lambda a, b: lax.dot_general(a, b, dims, preferred_element_type=F32)
    return (dot(left[0], right[1]) + dot(left[1], right[0])) + dot(left[0], right[0])


def same_index(size):
    rows = lax.broadcasted_iota(jnp.int32, (size, size), 0)
    return rows == lax.broadcasted_iota(jnp.int32, (size, size), 1)


def shifted_apply(diag, onsite, own, shifted):
    size = onsite.shape[1]
    shifted[...] = diag[0]
    for b in range(onsite.shape[0]):
        at = (pl.ds(b * size, size), pl.ds(b * size, size))
        shifted[at] += jnp.where(same_index(size), onsite[b : b + 1, :] - 2.0, 0.0)
    return product(split(shifted[...]), split(own))


def first_kernel(
    own_places, far_places, diag, onsite, own, tiles, far, first, high, low, block, shifted
):
    rows, states = own.shape
    colours, count, size, _ = tiles.shape
    halves = states // LANES
    result = shifted_apply(diag, onsite, own[...], shifted)
    for c in range(colours):
        block[...] = jnp.zeros_like(block)
        for k in range(count):
            block[own_places[c, 0, k], own_places[c, 1, k]] += tiles[c, k]
        for k in range(count):
            tile = far[c, pl.ds(rows * halves + k * size, size), :]
            block[far_places[c, 1, k], far_places[c, 0, k]] += tile.T
        for r in range(block.shape[0]):
            for s in range(block.shape[1]):
                at = (c, pl.ds(r * size, size), pl.ds(s * size, size))
                high[at], low[at] = split(block[r, s])
        mate = jnp.concatenate([far[c, pl.ds(h * rows, rows), :] for h in range(halves)], axis=1)
        result += product((high[c], low[c]), split(mate))
    first[...] = result * 0.25


def second_kernel(diag, onsite, own, high, low, far, base, filtered, gram, shifted):
    result = shifted_apply(diag, onsite, own[...], shifted)
    for c in range(high.shape[0]):
        result += product((high[c], low[c]), split(far[c]))
    value = result * 0.5 - base[...]
    filtered[...] = value
    parts = split(value)
    gram[...] = product(parts, parts, TN)


def finish_kernel(order, gram, filtered, basis, scaled):
    eye = same_index(gram.shape[0])
    total_gram = gram[...]
    scaled[...] = total_gram / order
    on_diag = jnp.where(eye, total_gram, 0.0)
    total = jnp.sum(jnp.sum(on_diag, axis=0, keepdims=True), axis=1, keepdims=True)
    half = jnp.where(eye, 1.5, 0.0)
    iterate = total_gram / total
    inverse = half - 0.5 * iterate
    parts = split(inverse)
    iterate = product(split(iterate), parts)
    for turn in range(1, NS_ITERS):
        held = parts
        moved = split(iterate)
        parts = split(half - 0.5 * product(held, moved))
        if turn < NS_ITERS - 1:
            iterate = product(moved, parts)
        inverse = product(parts, held)
        parts = split(inverse)
    scale = lax.sqrt(jnp.full_like(total, order)) / lax.sqrt(total)
    basis[...] = product(split(filtered[...]), parts) * scale


def call(kernel, outs, operands, scratch=(), scalars=0):
    return pl.pallas_call(
        kernel,
        out_shape=tuple(jax.ShapeDtypeStruct(shape, dtype) for shape, dtype in outs),
        in_specs=[SMEM] * scalars + [VMEM] * (len(operands) - scalars),
        out_specs=(VMEM,) * len(outs),
        scratch_shapes=[pltpu.VMEM(shape, F32) for shape in scratch],
    )(*operands)


def sum_over_devices(gram):
    core_bit = 3
    core = lax.axis_index("gx") & 1
    half = gram.shape[0] // 2
    keep = lax.dynamic_slice_in_dim(gram, core * half, half, 0)
    send = lax.dynamic_slice_in_dim(gram, (1 - core) * half, half, 0)
    value = keep + swap(send, 1 << core_bit)
    for flips in ((1, 2, 3), (4, 16, 20), (32, 64, 96)):
        others = [swap(value, flip) for flip in flips]
        value = (value + others[0]) + (others[1] + others[2])
    other = swap(value, 1 << core_bit)
    return jnp.where(
        core == 1, jnp.concatenate([other, value]), jnp.concatenate([value, other])
    )


def on_device(subspace, diag_blocks, onsite, coupling, tile_rows, tile_cols, partner):
    colours = partner.shape[0]
    rows, states = subspace.shape
    count, size = coupling.shape[2:4]
    tiles = coupling[:, 0]
    onsite = onsite.reshape(rows // size, size)
    masks = partner[:, 0]
    places = jnp.concatenate([tile_rows, tile_cols], axis=1)
    coded = jnp.pad(places.astype(F32), ((0, 0), (0, 6), (0, LANES - count)))
    columns = [subspace[:, h : h + LANES] for h in range(0, states, LANES)]

    def send_all(carry, colour):
        mask, own_tiles, own_places = colour
        payload = jnp.concatenate([*columns, own_tiles, own_places])
        return carry, exchange(mask, payload)

    stacked = tiles.reshape(colours, count * size, LANES)
    _, far = lax.scan(send_all, None, (masks, stacked, coded))
    far_places = far[:, -8:-6, :count].astype(jnp.int32)
    wide = ((rows, states), F32)
    parts = ((colours, rows, rows), BF16)
    blocks = rows // size
    first, high, low = call(
        first_kernel,
        (wide, parts, parts),
        (places, far_places, diag_blocks, onsite, subspace, tiles, far),
        ((blocks, blocks, size, size), (rows, rows)),
        scalars=2,
    )
    _, far = lax.scan(lambda carry, mask: (carry, exchange(mask, first)), None, masks)
    filtered, gram = call(
        second_kernel,
        (wide, ((states, states), F32)),
        (diag_blocks, onsite, first, high, low, far, subspace),
        ((rows, rows),),
    )
    order = float(rows * devices())
    return call(
        functools.partial(finish_kernel, order),
        (wide, ((states, states), F32)),
        (sum_over_devices(gram), filtered),
    )


def solution(mesh):
    placed = (
        P(AXES, None),
        P(AXES, None, None),
        P(AXES),
        P(None, AXES, None, None, None),
        P(None, AXES, None),
        P(None, AXES, None),
        P(),
    )
    return jax.shard_map(
        on_device,
        mesh=mesh,
        in_specs=placed,
        out_specs=(P(AXES, None), P()),
        check_vma=False,
    )
```

```python
import functools

import jax
import jax.numpy as jnp
from jax import lax
from jax.experimental import pallas as pl
from jax.experimental.pallas import tpu as pltpu
from jax.sharding import PartitionSpec as P

NS_ITERS = 12
AXES = ("gx", "gy")
VMEM = pl.BlockSpec(memory_space=pltpu.VMEM)
SMEM = pl.BlockSpec(memory_space=pltpu.SMEM)
F32 = jnp.float32
BF16 = jnp.bfloat16
LANES = 128
NN = (((1,), (0,)), ((), ()))
TN = (((0,), (0,)), ((), ()))


def devices():
    return lax.axis_size("gx") * lax.axis_size("gy")


def swap(value, flip):
    return lax.ppermute(value, AXES, [(i, i ^ flip) for i in range(devices())])


def exchange(mask, value):
    core = lax.axis_size("gy")
    keep = lambda kept: kept
    chips = [flip for flip in range(devices()) if not flip & core]
    movers = [functools.partial(swap, flip=flip) if flip else keep for flip in chips]
    place = (mask & (core - 1)) | ((mask // (2 * core)) * core)
    value = lax.switch(place, movers, value)
    return lax.cond((mask & core) != 0, functools.partial(swap, flip=core), keep, value)


def split(value):
    high = value.astype(BF16)
    return high, (value - high.astype(F32)).astype(BF16)


def product(left, right, dims=NN):
    dot = lambda a, b: lax.dot_general(a, b, dims, preferred_element_type=F32)
    return (dot(left[0], right[1]) + dot(left[1], right[0])) + dot(left[0], right[0])


def same_index(size):
    rows = lax.broadcasted_iota(jnp.int32, (size, size), 0)
    return rows == lax.broadcasted_iota(jnp.int32, (size, size), 1)


def prepare_kernel(places, diag, onsite, own, tiles, high, low, acc, payload, block, mirror):
    rows = own.shape[0]
    colours, count, size, _ = tiles.shape
    corners = range(rows // size)
    for c in range(colours):
        block[...] = jnp.zeros_like(block)
        mirror[...] = jnp.zeros_like(mirror)
        for k in range(count):
            tile = tiles[c, k]
            block[places[c, 0, k], places[c, 1, k]] += tile
            mirror[places[c, 1, k], places[c, 0, k]] += tile.T
        for r in corners:
            for s in corners:
                at = (pl.ds(r * size, size), pl.ds(s * size, size))
                high[(c, *at)], low[(c, *at)] = split(block[r, s])
                high[(colours + c, *at)], low[(colours + c, *at)] = split(mirror[r, s])
    for r in corners:
        for s in corners:
            at = (pl.ds(r * size, size), pl.ds(s * size, size))
            value = diag[(0, *at)]
            if r == s:
                value += jnp.where(same_index(size), onsite[r : r + 1, :] - 2.0, 0.0)
            high[(2 * colours, *at)], low[(2 * colours, *at)] = split(value)
    value = own[...]
    parts = split(value)
    acc[...] = product((high[2 * colours], low[2 * colours]), parts)
    payload[pl.ds(0, rows), :] = value
    payload[pl.ds(rows, rows), :] = product((high[colours], low[colours]), parts)


def step_kernel(turn, high, low, own, got, held_acc, held, acc, payload):
    rows = own.shape[0]
    top, bottom = pl.ds(0, rows), pl.ds(rows, rows)
    colours = (high.shape[0] - 1) // 2
    now = turn[0]
    colour = lax.rem(now, colours)
    last = colours * 2 - 1
    mate = split(got[top, :])
    acc[...] = held_acc[...] + got[bottom, :] + product((high[colour], low[colour]), mate)
    payload[top, :] = held[top, :]

    @pl.when(now == colours - 1)
    def _():
        value = acc[...] * 0.25
        payload[top, :] = value
        acc[...] = product((high[2 * colours], low[2 * colours]), split(value))

    @pl.when(now == last)
    def _():
        payload[top, :] = acc[...] * 0.5 - own[...]

    @pl.when(now < last)
    def _():
        following = colours + lax.rem(now + 1, colours)
        parts = split(payload[top, :])
        payload[bottom, :] = product((high[following], low[following]), parts)


def gram_kernel(payload, filtered, gram):
    value = payload[pl.ds(0, filtered.shape[0]), :]
    filtered[...] = value
    parts = split(value)
    gram[...] = product(parts, parts, TN)


def finish_kernel(order, gram, filtered, basis, scaled):
    eye = same_index(gram.shape[0])
    total_gram = gram[...]
    scaled[...] = total_gram / order
    on_diag = jnp.where(eye, total_gram, 0.0)
    total = jnp.sum(jnp.sum(on_diag, axis=0, keepdims=True), axis=1, keepdims=True)
    half = jnp.where(eye, 1.5, 0.0)
    iterate = total_gram / total
    inverse = half - 0.5 * iterate
    parts = split(inverse)
    iterate = product(split(iterate), parts)
    for turn in range(1, NS_ITERS):
        held = parts
        moved = split(iterate)
        parts = split(half - 0.5 * product(held, moved))
        if turn < NS_ITERS - 1:
            iterate = product(moved, parts)
        inverse = product(parts, held)
        parts = split(inverse)
    scale = lax.sqrt(jnp.full_like(total, order)) / lax.sqrt(total)
    basis[...] = product(split(filtered[...]), parts) * scale


def call(kernel, outs, operands, scratch=(), scalars=0, aliases=None):
    return pl.pallas_call(
        kernel,
        out_shape=tuple(jax.ShapeDtypeStruct(shape, dtype) for shape, dtype in outs),
        in_specs=[SMEM] * scalars + [VMEM] * (len(operands) - scalars),
        out_specs=(VMEM,) * len(outs),
        scratch_shapes=[pltpu.VMEM(shape, F32) for shape in scratch],
        input_output_aliases=aliases or {},
    )(*operands)


def sum_over_devices(gram):
    core_bit = 3
    core = lax.axis_index("gx") & 1
    half = gram.shape[0] // 2
    keep = lax.dynamic_slice_in_dim(gram, core * half, half, 0)
    send = lax.dynamic_slice_in_dim(gram, (1 - core) * half, half, 0)
    value = keep + swap(send, 1 << core_bit)
    for flips in ((1, 2, 3), (4, 16, 20), (32, 64, 96)):
        others = [swap(value, flip) for flip in flips]
        value = (value + others[0]) + (others[1] + others[2])
    other = swap(value, 1 << core_bit)
    return jnp.where(
        core == 1, jnp.concatenate([other, value]), jnp.concatenate([value, other])
    )


def on_device(subspace, diag_blocks, onsite, coupling, tile_rows, tile_cols, partner):
    colours = partner.shape[0]
    rows, states = subspace.shape
    size = coupling.shape[3]
    blocks = rows // size
    places = jnp.concatenate([tile_rows, tile_cols], axis=1)
    masks = partner[:, 0]
    wide, double = ((rows, states), F32), ((2 * rows, states), F32)
    square = ((states, states), F32)
    parts = ((2 * colours + 1, rows, rows), BF16)
    high, low, acc, payload = call(
        prepare_kernel,
        (parts, parts, wide, double),
        (places, diag_blocks, onsite.reshape(blocks, size), subspace, coupling[:, 0]),
        ((blocks, blocks, size, size),) * 2,
        scalars=1,
    )

    def step(turn, state):
        acc, payload = state
        got = exchange(masks[turn % colours], payload)
        return call(
            step_kernel,
            (wide, double),
            (turn.reshape(1), high, low, subspace, got, acc, payload),
            scalars=1,
            aliases={5: 0, 6: 1},
        )

    acc, payload = lax.fori_loop(0, 2 * colours, step, (acc, payload))
    filtered, gram = call(gram_kernel, (wide, square), (payload,))
    order = float(rows * devices())
    return call(
        functools.partial(finish_kernel, order),
        (wide, square),
        (sum_over_devices(gram), filtered),
    )


def solution(mesh):
    placed = (
        P(AXES, None),
        P(AXES, None, None),
        P(AXES),
        P(None, AXES, None, None, None),
        P(None, AXES, None),
        P(None, AXES, None),
        P(),
    )
    return jax.shard_map(
        on_device,
        mesh=mesh,
        in_specs=placed,
        out_specs=(P(AXES, None), P()),
        check_vma=False,
    )
```

```python
import functools

import jax
import jax.numpy as jnp
from jax import lax
from jax.experimental import pallas as pl
from jax.experimental.pallas import tpu as pltpu
from jax.sharding import PartitionSpec as P

NS_ITERS = 12
AXES = ("gx", "gy")
VMEM = pl.BlockSpec(memory_space=pltpu.VMEM)
FAR = pl.BlockSpec(memory_space=pl.ANY)
SMEM = pl.BlockSpec(memory_space=pltpu.SMEM)
F32 = jnp.float32
BF16 = jnp.bfloat16
PAD = 16
VMEM_LIMIT = 28 << 20
NN = (((1,), (0,)), ((), ()))
TN = (((0,), (0,)), ((), ()))


def devices():
    return lax.axis_size("gx") * lax.axis_size("gy")


def swap(value, flip):
    return lax.ppermute(value, AXES, [(i, i ^ flip) for i in range(devices())])


def route(mask, core):
    above = lax.shift_right_logical(mask, jnp.int32(core.bit_length()))
    return (mask & (core - 1)) | (above * core), jnp.where((mask & core) != 0, 1, 0)


def exchange(place, flips_core, value):
    core = lax.axis_size("gy")
    keep = lambda kept: kept
    chips = [flip for flip in range(devices()) if not flip & core]
    movers = [functools.partial(swap, flip=flip) if flip else keep for flip in chips]
    value = lax.switch(place, movers, value)
    return lax.switch(flips_core, [keep, functools.partial(swap, flip=core)], value)


def split(value):
    high = value.astype(BF16)
    return high, (value - high.astype(F32)).astype(BF16)


def product(left, right, dims=NN):
    dot = lambda a, b: lax.dot_general(a, b, dims, preferred_element_type=F32)
    return (dot(left[0], right[1]) + dot(left[1], right[0])) + dot(left[0], right[0])


def indices(size):
    return tuple(lax.broadcasted_iota(jnp.int32, (size, size), axis) for axis in range(2))


def same_index(size):
    row, column = indices(size)
    return row == column


def prepare_kernel(
    core, tile_rows, tile_cols, partner, diag, onsite, own, tiles,
    high, low, acc, payload, place, flips_core, block, mirror,
):
    rows = own.shape[0]
    colours, count, size, _ = tiles.shape
    corners = range(rows // size)
    place[0], flips_core[0] = route(partner[0, 0], core)
    for c in range(colours):
        block[...] = jnp.zeros_like(block)
        mirror[...] = jnp.zeros_like(mirror)
        for k in range(count):
            tile = tiles[c, k]
            r, s = tile_rows[c, 0, k], tile_cols[c, 0, k]
            block[r, s] += tile
            mirror[s, r] += tile.T
        for r in corners:
            for s in corners:
                at = (pl.ds(r * size, size), pl.ds(s * size, size))
                high[(c, *at)], low[(c, *at)] = split(block[r, s])
                high[(colours + c, *at)], low[(colours + c, *at)] = split(mirror[r, s])
    for r in corners:
        for s in corners:
            at = (pl.ds(r * size, size), pl.ds(s * size, size))
            value = diag[(0, *at)]
            if r == s:
                value += jnp.where(same_index(size), onsite[r : r + 1, :] - 2.0, 0.0)
            high[(2 * colours, *at)], low[(2 * colours, *at)] = split(value)
    value = own[...]
    parts = split(value)
    acc[...] = product((high[2 * colours], low[2 * colours]), parts)
    payload[pl.ds(0, rows), :] = value
    payload[pl.ds(rows, rows), :] = product((high[colours], low[colours]), parts)


def step_kernel(
    core, turn, partner, high, low, own, got, held_acc, held,
    acc, payload, place, flips_core, near_high, near_low, sems,
):
    rows = own.shape[0]
    top, bottom = pl.ds(0, rows), pl.ds(rows, rows)
    colours = (high.shape[0] - 1) // 2
    now = turn[0]
    colour, following = lax.rem(now, colours), lax.rem(now + 1, colours)
    last = colours * 2 - 1

    def fetch(index, slot):
        pairs = ((high, near_high), (low, near_low))
        return [
            pltpu.make_async_copy(far.at[index], near.at[slot], sems.at[slot, part])
            for part, (far, near) in enumerate(pairs)
        ]

    def fetched(copies, slot):
        for copy in copies:
            copy.wait()
        return near_high[slot], near_low[slot]

    forward, backward = fetch(colour, 0), fetch(colours + following, 1)
    diagonal = fetch(2 * colours, 2)
    for copy in forward + backward:
        copy.start()

    @pl.when(now == colours - 1)
    def _():
        for copy in diagonal:
            copy.start()

    place[0], flips_core[0] = route(partner[following, 0], core)
    mate = split(got[top, :])
    acc[...] = held_acc[...] + got[bottom, :] + product(fetched(forward, 0), mate)
    payload[top, :] = held[top, :]

    @pl.when(now == colours - 1)
    def _():
        value = acc[...] * 0.25
        payload[top, :] = value
        acc[...] = product(fetched(diagonal, 2), split(value))

    @pl.when(now == last)
    def _():
        payload[top, :] = acc[...] * 0.5 - own[...]

    turned = fetched(backward, 1)

    @pl.when(now < last)
    def _():
        payload[bottom, :] = product(turned, split(payload[top, :]))


def gram_kernel(second_core, payload, keep, send, packed):
    states = payload.shape[1]
    half = states // 2
    parts = split(payload[pl.ds(0, payload.shape[0] // 2), :])
    gram = product(parts, parts, TN)
    row, column = indices(half)
    lower = gram[half:, half:]
    packed[pl.ds(0, half), :] = jnp.concatenate(
        [jnp.where(row <= column, gram[:half, :half], lower), gram[:half, half:]], axis=1
    )
    diagonal = jnp.sum(jnp.where(row == column, lower, 0.0), axis=0, keepdims=True)
    packed[pl.ds(half, PAD), :] = jnp.broadcast_to(
        jnp.concatenate([diagonal, diagonal], axis=1), (PAD, states)
    )
    share = packed.shape[0] // 2
    for own in range(2):

        @pl.when(second_core[0] == own)
        def _():
            keep[...] = packed[pl.ds(own * share, share), :]
            send[...] = packed[pl.ds((1 - own) * share, share), :]


def unpack_gram(second_core, value, other, packed):
    share = value.shape[0]
    for own in range(2):

        @pl.when(second_core[0] == own)
        def _():
            packed[pl.ds(own * share, share), :] = value[...]
            packed[pl.ds((1 - own) * share, share), :] = other[...]

    half = value.shape[1] // 2
    mixed, corner = packed[pl.ds(0, half), :half], packed[pl.ds(0, half), half:]
    turned = mixed.T
    row, column = indices(half)
    first = jnp.where(row <= column, mixed, turned)
    second = jnp.where(row > column, mixed, turned)
    second = jnp.where(row == column, packed[pl.ds(half, 1), :half], second)
    return jnp.concatenate(
        [jnp.concatenate([first, corner], axis=1), jnp.concatenate([corner.T, second], axis=1)],
        axis=0,
    )


def finish_kernel(order, second_core, value, other, payload, basis, scaled, packed):
    total_gram = unpack_gram(second_core, value, other, packed)
    scaled[...] = total_gram / order
    row, column = indices(total_gram.shape[0])
    eye = row == column
    on_diag = jnp.where(eye, total_gram, 0.0)
    total = jnp.sum(jnp.sum(on_diag, axis=0, keepdims=True), axis=1, keepdims=True)
    half = jnp.where(eye, 1.5, 0.0)
    iterate = total_gram / total
    inverse = half - 0.5 * iterate
    parts = split(inverse)
    iterate = product(split(iterate), parts)
    for turn in range(1, NS_ITERS):
        held = parts
        moved = split(iterate)
        parts = split(half - 0.5 * product(held, moved))
        if turn < NS_ITERS - 1:
            iterate = product(moved, parts)
        inverse = product(parts, held)
        parts = split(inverse)
    scale = lax.sqrt(jnp.full_like(total, order)) / lax.sqrt(total)
    rows = basis.shape[0]
    basis[...] = product(split(payload[pl.ds(0, rows), :]), parts) * scale


def call(kernel, outs, operands, scratch=(), scalars=0, far=0, routes=0, aliases=None):
    shapes = tuple(jax.ShapeDtypeStruct(shape, dtype) for shape, dtype in outs)
    shapes += (jax.ShapeDtypeStruct((1,), jnp.int32),) * routes
    return pl.pallas_call(
        kernel,
        out_shape=shapes,
        in_specs=[SMEM] * scalars + [FAR] * far + [VMEM] * (len(operands) - scalars - far),
        out_specs=(VMEM,) * len(outs) + (SMEM,) * routes,
        scratch_shapes=[pltpu.VMEM(s, F32) if isinstance(s, tuple) else s for s in scratch],
        input_output_aliases=aliases or {},
        compiler_params=pltpu.CompilerParams(vmem_limit_bytes=VMEM_LIMIT),
    )(*operands)


def sum_over_devices(keep, send):
    value = keep + swap(send, lax.axis_size("gy"))
    for flips in ((1, 3, 2), (4, 20, 16), (32, 96, 64)):
        others = [swap(value, flip) for flip in flips]
        value = (value + others[0]) + (others[1] + others[2])
    return value, swap(value, lax.axis_size("gy"))


def on_device(subspace, diag_blocks, onsite, coupling, tile_rows, tile_cols, partner):
    colours = partner.shape[0]
    rows, states = subspace.shape
    size = coupling.shape[3]
    blocks = rows // size
    core = lax.axis_size("gy")
    wide, double = ((rows, states), F32), ((2 * rows, states), F32)
    parts = ((2 * colours + 1, rows, rows), BF16)
    high, low, *state = call(
        functools.partial(prepare_kernel, core),
        (parts, parts, wide, double),
        (
            tile_rows, tile_cols, partner,
            diag_blocks, onsite.reshape(blocks, size), subspace, coupling[:, 0],
        ),
        ((blocks, blocks, size, size),) * 2,
        scalars=3,
        routes=2,
    )

    def step(turn, state):
        acc, payload, place, flips_core = state
        got = exchange(place[0], flips_core[0], payload)
        return call(
            functools.partial(step_kernel, core),
            (wide, double),
            (turn.reshape(1), partner, high, low, subspace, got, acc, payload),
            (*(pltpu.VMEM((3, rows, rows), BF16),) * 2, pltpu.SemaphoreType.DMA((3, 2))),
            scalars=2,
            far=2,
            routes=2,
            aliases={6: 0, 7: 1},
        )

    _, payload, _, _ = lax.fori_loop(0, 2 * colours, step, tuple(state))
    second_core = (lax.axis_index("gx") & 1).reshape(1)
    packed = (states // 2 + PAD, states)
    share = ((packed[0] // 2, states), F32)
    keep, send = call(gram_kernel, (share, share), (second_core, payload), (packed,), scalars=1)
    return call(
        functools.partial(finish_kernel, float(rows * devices())),
        (wide, ((states, states), F32)),
        (second_core, *sum_over_devices(keep, send), payload),
        (packed,),
        scalars=1,
    )


def solution(mesh):
    placed = (
        P(AXES, None),
        P(AXES, None, None),
        P(AXES),
        P(None, AXES, None, None, None),
        P(None, AXES, None),
        P(None, AXES, None),
        P(),
    )
    return jax.shard_map(
        on_device,
        mesh=mesh,
        in_specs=placed,
        out_specs=(P(AXES, None), P()),
        check_vma=False,
    )
```

```python
import functools

import jax
import jax.numpy as jnp
from jax import lax
from jax.experimental import pallas as pl
from jax.experimental.pallas import tpu as pltpu
from jax.sharding import PartitionSpec as P

NS_ITERS = 12
AXES = ("gx", "gy")
VMEM = pl.BlockSpec(memory_space=pltpu.VMEM)
FAR = pl.BlockSpec(memory_space=pl.ANY)
SMEM = pl.BlockSpec(memory_space=pltpu.SMEM)
F32 = jnp.float32
BF16 = jnp.bfloat16
PAD = 16
VMEM_LIMIT = 28 << 20
NN = (((1,), (0,)), ((), ()))
TN = (((0,), (0,)), ((), ()))


def devices():
    return lax.axis_size("gx") * lax.axis_size("gy")


def swap(value, flip):
    return lax.ppermute(value, AXES, [(i, i ^ flip) for i in range(devices())])


def route(mask, core):
    above = lax.shift_right_logical(mask, jnp.int32(core.bit_length()))
    return (mask & (core - 1)) | (above * core), jnp.where((mask & core) != 0, 1, 0)


def exchange(place, flips_core, value):
    core = lax.axis_size("gy")
    keep = lambda kept: kept
    chips = [flip for flip in range(devices()) if not flip & core]
    movers = [functools.partial(swap, flip=flip) if flip else keep for flip in chips]
    value = lax.switch(place, movers, value)
    return lax.switch(flips_core, [keep, functools.partial(swap, flip=core)], value)


def split(value):
    high = value.astype(BF16)
    return high, (value - high.astype(F32)).astype(BF16)


def product(left, right, dims=NN):
    dot = lambda a, b: lax.dot_general(a, b, dims, preferred_element_type=F32)
    return (dot(left[0], right[1]) + dot(left[1], right[0])) + dot(left[0], right[0])


def stacked(left, right):
    dot = lambda a, b: lax.dot_general(a, b, NN, preferred_element_type=F32)
    rows = left[0].shape[0]
    both = dot(jnp.concatenate(left, axis=0), right[0])
    return (dot(left[0], right[1]) + both[rows:]) + both[:rows]


def indices(size):
    return tuple(lax.broadcasted_iota(jnp.int32, (size, size), axis) for axis in range(2))


def same_index(size):
    row, column = indices(size)
    return row == column


def prepare_kernel(
    core, tile_rows, tile_cols, partner, diag, onsite, own, tiles,
    high, low, acc, payload, place, flips_core, block, mirror,
):
    rows = own.shape[0]
    colours, count, size, _ = tiles.shape
    corners = range(rows // size)
    place[0], flips_core[0] = route(partner[0, 0], core)
    for c in range(colours):
        block[...] = jnp.zeros_like(block)
        mirror[...] = jnp.zeros_like(mirror)
        for k in range(count):
            tile = tiles[c, k]
            r, s = tile_rows[c, 0, k], tile_cols[c, 0, k]
            block[r, s] += tile
            mirror[s, r] += tile.T
        for r in corners:
            for s in corners:
                at = (pl.ds(r * size, size), pl.ds(s * size, size))
                high[(c, *at)], low[(c, *at)] = split(block[r, s])
                high[(colours + c, *at)], low[(colours + c, *at)] = split(mirror[r, s])
    for r in corners:
        for s in corners:
            at = (pl.ds(r * size, size), pl.ds(s * size, size))
            value = diag[(0, *at)]
            if r == s:
                value += jnp.where(same_index(size), onsite[r : r + 1, :] - 2.0, 0.0)
            high[(2 * colours, *at)], low[(2 * colours, *at)] = split(value)
    value = own[...]
    parts = split(value)
    acc[...] = product((high[2 * colours], low[2 * colours]), parts)
    payload[pl.ds(0, rows), :] = value
    payload[pl.ds(rows, rows), :] = product((high[colours], low[colours]), parts)


def step_kernel(
    core, turn, partner, high, low, got, own, held_acc, held,
    acc, payload, place, flips_core, near_high, near_low, near, sems, near_sems,
):
    rows = own.shape[0]
    top, bottom = pl.ds(0, rows), pl.ds(rows, rows)
    colours = (high.shape[0] - 1) // 2
    now = turn[0]
    colour, following = lax.rem(now, colours), lax.rem(now + 1, colours)
    last = colours * 2 - 1

    def fetch(index, slot):
        pairs = ((high, near_high), (low, near_low))
        return [
            pltpu.make_async_copy(far.at[index], close.at[slot], sems.at[slot, part])
            for part, (far, close) in enumerate(pairs)
        ]

    def fetched(copies, slot):
        for copy in copies:
            copy.wait()
        return near_high[slot], near_low[slot]

    backward, forward = fetch(colours + following, 0), fetch(colour, 1)
    diagonal = fetch(2 * colours, 2)
    arrived = [
        pltpu.make_async_copy(got.at[half], near.at[half], near_sems.at[part])
        for part, half in enumerate((top, bottom))
    ]
    for copy in backward + arrived[:1] + forward + arrived[1:]:
        copy.start()
    ends = colour == colours - 1

    @pl.when(now == colours - 1)
    def _():
        for copy in diagonal:
            copy.start()

    place[0], flips_core[0] = route(partner[following, 0], core)
    turned = fetched(backward, 0)

    @pl.when(jnp.logical_not(ends))
    def _():
        value = held[top, :]
        payload[top, :] = value
        payload[bottom, :] = product(turned, split(value))

    arrived[0].wait()
    terms = product(fetched(forward, 1), split(near[top, :]))
    arrived[1].wait()
    acc[...] = (held_acc[...] + near[bottom, :]) + terms

    @pl.when(now == colours - 1)
    def _():
        value = acc[...] * 0.25
        parts = split(value)
        payload[top, :] = value
        acc[...] = product(fetched(diagonal, 2), parts)
        payload[bottom, :] = product(turned, parts)

    @pl.when(now == last)
    def _():
        payload[top, :] = acc[...] * 0.5 - own[...]


def gram_kernel(second_core, payload, keep, send, packed):
    states = payload.shape[1]
    half = states // 2
    parts = split(payload[pl.ds(0, payload.shape[0] // 2), :])
    gram = product(parts, parts, TN)
    row, column = indices(half)
    lower = gram[half:, half:]
    packed[pl.ds(0, half), :] = jnp.concatenate(
        [jnp.where(row <= column, gram[:half, :half], lower), gram[:half, half:]], axis=1
    )
    diagonal = jnp.sum(jnp.where(row == column, lower, 0.0), axis=0, keepdims=True)
    packed[pl.ds(half, PAD), :] = jnp.broadcast_to(
        jnp.concatenate([diagonal, diagonal], axis=1), (PAD, states)
    )
    share = packed.shape[0] // 2
    for own in range(2):

        @pl.when(second_core[0] == own)
        def _():
            keep[...] = packed[pl.ds(own * share, share), :]
            send[...] = packed[pl.ds((1 - own) * share, share), :]


def unpack_gram(second_core, value, other, packed):
    share = value.shape[0]
    for own in range(2):

        @pl.when(second_core[0] == own)
        def _():
            packed[pl.ds(own * share, share), :] = value[...]
            packed[pl.ds((1 - own) * share, share), :] = other[...]

    half = value.shape[1] // 2
    mixed, corner = packed[pl.ds(0, half), :half], packed[pl.ds(0, half), half:]
    turned = mixed.T
    row, column = indices(half)
    first = jnp.where(row <= column, mixed, turned)
    second = jnp.where(row > column, mixed, turned)
    second = jnp.where(row == column, packed[pl.ds(half, 1), :half], second)
    return jnp.concatenate(
        [jnp.concatenate([first, corner], axis=1), jnp.concatenate([corner.T, second], axis=1)],
        axis=0,
    )


def finish_kernel(order, second_core, value, other, payload, basis, scaled, packed):
    total_gram = unpack_gram(second_core, value, other, packed)
    scaled[...] = total_gram / order
    row, column = indices(total_gram.shape[0])
    eye = row == column
    on_diag = jnp.where(eye, total_gram, 0.0)
    total = jnp.sum(jnp.sum(on_diag, axis=0, keepdims=True), axis=1, keepdims=True)
    half = jnp.where(eye, 1.5, 0.0)
    iterate = total_gram / total
    inverse = half - 0.5 * iterate
    parts = split(inverse)
    iterate = stacked(split(iterate), parts)
    for turn in range(1, NS_ITERS):
        held = parts
        moved = split(iterate)
        parts = split(half - 0.5 * stacked(held, moved))
        if turn < NS_ITERS - 1:
            iterate = stacked(moved, parts)
        inverse = stacked(parts, held)
        parts = split(inverse)
    scale = lax.sqrt(jnp.full_like(total, order)) / lax.sqrt(total)
    rows = basis.shape[0]
    basis[...] = stacked(split(payload[pl.ds(0, rows), :]), parts) * scale


def call(kernel, outs, operands, scratch=(), scalars=0, far=0, routes=0, aliases=None, limit=VMEM_LIMIT):
    shapes = tuple(jax.ShapeDtypeStruct(shape, dtype) for shape, dtype in outs)
    shapes += (jax.ShapeDtypeStruct((1,), jnp.int32),) * routes
    return pl.pallas_call(
        kernel,
        out_shape=shapes,
        in_specs=[SMEM] * scalars + [FAR] * far + [VMEM] * (len(operands) - scalars - far),
        out_specs=(VMEM,) * len(outs) + (SMEM,) * routes,
        scratch_shapes=[pltpu.VMEM(s, F32) if isinstance(s, tuple) else s for s in scratch],
        input_output_aliases=aliases or {},
        compiler_params=pltpu.CompilerParams(vmem_limit_bytes=limit),
    )(*operands)


def sum_over_devices(keep, send):
    value = keep + swap(send, lax.axis_size("gy"))
    for flips in ((1, 3, 2), (4, 20, 16), (32, 96, 64)):
        others = [swap(value, flip) for flip in flips]
        value = (value + others[0]) + (others[1] + others[2])
    return value, swap(value, lax.axis_size("gy"))


def on_device(subspace, diag_blocks, onsite, coupling, tile_rows, tile_cols, partner):
    colours = partner.shape[0]
    rows, states = subspace.shape
    size = coupling.shape[3]
    blocks = rows // size
    core = lax.axis_size("gy")
    wide, double = ((rows, states), F32), ((2 * rows, states), F32)
    parts = ((2 * colours + 1, rows, rows), BF16)
    high, low, *state = call(
        functools.partial(prepare_kernel, core),
        (parts, parts, wide, double),
        (
            tile_rows, tile_cols, partner,
            diag_blocks, onsite.reshape(blocks, size), subspace, coupling[:, 0],
        ),
        ((blocks, blocks, size, size),) * 2,
        scalars=3,
        routes=2,
        limit=None,
    )

    def step(turn, state):
        acc, payload, place, flips_core = state
        got = exchange(place[0], flips_core[0], payload)
        return call(
            functools.partial(step_kernel, core),
            (wide, double),
            (turn.reshape(1), partner, high, low, got, subspace, acc, payload),
            (
                *(pltpu.VMEM((3, rows, rows), BF16),) * 2,
                (2 * rows, states),
                pltpu.SemaphoreType.DMA((3, 2)),
                pltpu.SemaphoreType.DMA((2,)),
            ),
            scalars=2,
            far=3,
            routes=2,
            aliases={6: 0, 7: 1},
        )

    _, payload, _, _ = lax.fori_loop(0, 2 * colours, step, tuple(state))
    second_core = (lax.axis_index("gx") & 1).reshape(1)
    packed = (states // 2 + PAD, states)
    share = ((packed[0] // 2, states), F32)
    keep, send = call(gram_kernel, (share, share), (second_core, payload), (packed,), scalars=1)
    return call(
        functools.partial(finish_kernel, float(rows * devices())),
        (wide, ((states, states), F32)),
        (second_core, *sum_over_devices(keep, send), payload),
        (packed,),
        scalars=1,
    )


def solution(mesh):
    placed = (
        P(AXES, None),
        P(AXES, None, None),
        P(AXES),
        P(None, AXES, None, None, None),
        P(None, AXES, None),
        P(None, AXES, None),
        P(),
    )
    return jax.shard_map(
        on_device,
        mesh=mesh,
        in_specs=placed,
        out_specs=(P(AXES, None), P()),
        check_vma=False,
    )
```

```python
import functools

import jax
import jax.numpy as jnp
from jax import lax
from jax.experimental import pallas as pl
from jax.experimental.pallas import tpu as pltpu
from jax.sharding import PartitionSpec as P

NS_ITERS = 12
AXES = ("gx", "gy")
VMEM = pl.BlockSpec(memory_space=pltpu.VMEM)
FAR = pl.BlockSpec(memory_space=pl.ANY)
SMEM = pl.BlockSpec(memory_space=pltpu.SMEM)
F32 = jnp.float32
BF16 = jnp.bfloat16
PAD = 16
VMEM_LIMIT = 28 << 20
NN = (((1,), (0,)), ((), ()))
TN = (((0,), (0,)), ((), ()))


def devices():
    return lax.axis_size("gx") * lax.axis_size("gy")


def swap(value, flip):
    return lax.ppermute(value, AXES, [(i, i ^ flip) for i in range(devices())])


def route(mask, core):
    above = lax.shift_right_logical(mask, jnp.int32(core.bit_length()))
    return (mask & (core - 1)) | (above * core), jnp.where((mask & core) != 0, 1, 0)


def exchange(place, flips_core, value):
    core = lax.axis_size("gy")
    keep = lambda kept: kept
    chips = [flip for flip in range(devices()) if not flip & core]
    movers = [functools.partial(swap, flip=flip) if flip else keep for flip in chips]
    value = lax.switch(place, movers, value)
    return lax.switch(flips_core, [keep, functools.partial(swap, flip=core)], value)


def split(value):
    high = value.astype(BF16)
    return high, (value - high.astype(F32)).astype(BF16)


def product(left, right, dims=NN):
    dot = lambda a, b: lax.dot_general(a, b, dims, preferred_element_type=F32)
    kept = 1 - dims[0][0][0]
    halves = zip(*(jnp.split(part, 2, axis=kept) for part in left))
    return jnp.concatenate(
        [
            (dot(high, right[1]) + dot(low, right[0])) + dot(high, right[0])
            for high, low in halves
        ],
        axis=0,
    )


def indices(size):
    return tuple(lax.broadcasted_iota(jnp.int32, (size, size), axis) for axis in range(2))


def same_index(size):
    row, column = indices(size)
    return row == column


def prepare_kernel(
    core, tile_rows, tile_cols, partner, diag, onsite, own, tiles,
    high, low, acc, payload, place, flips_core, block,
):
    rows = own.shape[0]
    colours, count, size, _ = tiles.shape
    corners = range(rows // size)
    place[0], flips_core[0] = route(partner[0, 0], core)
    for c in range(colours):
        block[...] = jnp.zeros_like(block)
        for k in range(count):
            block[tile_rows[c, 0, k], tile_cols[c, 0, k]] += tiles[c, k]
        for r in corners:
            for s in corners:
                at = (pl.ds(r * size, size), pl.ds(s * size, size))
                high[(c, *at)], low[(c, *at)] = split(block[r, s])
    for r in corners:
        for s in corners:
            at = (pl.ds(r * size, size), pl.ds(s * size, size))
            value = diag[(0, *at)]
            if r == s:
                value += jnp.where(same_index(size), onsite[r : r + 1, :] - 2.0, 0.0)
            high[(colours, *at)], low[(colours, *at)] = split(value)
    value = own[...]
    parts = split(value)
    acc[...] = product((high[colours], low[colours]), parts)
    payload[pl.ds(0, rows), :] = value
    payload[pl.ds(rows, rows), :] = product((high[0], low[0]), parts, TN)


def step_kernel(
    core, turn, partner, high, low, got, own, held_acc, held,
    acc, payload, place, flips_core, near_high, near_low, near, sems, near_sems,
):
    rows = own.shape[0]
    top, bottom = pl.ds(0, rows), pl.ds(rows, rows)
    colours = high.shape[0] - 1
    now = turn[0]
    colour, following = lax.rem(now, colours), lax.rem(now + 1, colours)
    last = colours * 2 - 1

    def fetch(index, slot):
        pairs = ((high, near_high), (low, near_low))
        return [
            pltpu.make_async_copy(far.at[index], close.at[slot], sems.at[slot, part])
            for part, (far, close) in enumerate(pairs)
        ]

    def fetched(copies, slot):
        for copy in copies:
            copy.wait()
        return near_high[slot], near_low[slot]

    backward, forward = fetch(following, 0), fetch(colour, 1)
    diagonal = fetch(colours, 2)
    arrived = [
        pltpu.make_async_copy(got.at[half], near.at[half], near_sems.at[part])
        for part, half in enumerate((top, bottom))
    ]
    for copy in backward + arrived[:1] + forward + arrived[1:]:
        copy.start()
    ends = colour == colours - 1

    @pl.when(now == colours - 1)
    def _():
        for copy in diagonal:
            copy.start()

    place[0], flips_core[0] = route(partner[following, 0], core)
    turned = fetched(backward, 0)

    @pl.when(jnp.logical_not(ends))
    def _():
        value = held[top, :]
        payload[top, :] = value
        payload[bottom, :] = product(turned, split(value), TN)

    arrived[0].wait()
    terms = product(fetched(forward, 1), split(near[top, :]))
    arrived[1].wait()
    acc[...] = (held_acc[...] + near[bottom, :]) + terms

    @pl.when(now == colours - 1)
    def _():
        value = acc[...] * 0.25
        parts = split(value)
        payload[top, :] = value
        acc[...] = product(fetched(diagonal, 2), parts)
        payload[bottom, :] = product(turned, parts, TN)

    @pl.when(now == last)
    def _():
        payload[top, :] = acc[...] * 0.5 - own[...]


def gram_kernel(second_core, payload, keep, send, packed):
    states = payload.shape[1]
    half = states // 2
    parts = split(payload[pl.ds(0, payload.shape[0] // 2), :])
    gram = product(parts, parts, TN)
    row, column = indices(half)
    lower = gram[half:, half:]
    packed[pl.ds(0, half), :] = jnp.concatenate(
        [jnp.where(row <= column, gram[:half, :half], lower), gram[:half, half:]], axis=1
    )
    diagonal = jnp.sum(jnp.where(row == column, lower, 0.0), axis=0, keepdims=True)
    packed[pl.ds(half, PAD), :] = jnp.broadcast_to(
        jnp.concatenate([diagonal, diagonal], axis=1), (PAD, states)
    )
    share = packed.shape[0] // 2
    for own in range(2):

        @pl.when(second_core[0] == own)
        def _():
            keep[...] = packed[pl.ds(own * share, share), :]
            send[...] = packed[pl.ds((1 - own) * share, share), :]


def unpack_gram(second_core, value, other, packed):
    share = value.shape[0]
    for own in range(2):

        @pl.when(second_core[0] == own)
        def _():
            packed[pl.ds(own * share, share), :] = value[...]
            packed[pl.ds((1 - own) * share, share), :] = other[...]

    half = value.shape[1] // 2
    mixed, corner = packed[pl.ds(0, half), :half], packed[pl.ds(0, half), half:]
    turned = mixed.T
    row, column = indices(half)
    first = jnp.where(row <= column, mixed, turned)
    second = jnp.where(row > column, mixed, turned)
    second = jnp.where(row == column, packed[pl.ds(half, 1), :half], second)
    return jnp.concatenate(
        [jnp.concatenate([first, corner], axis=1), jnp.concatenate([corner.T, second], axis=1)],
        axis=0,
    )


def finish_kernel(order, second_core, value, other, payload, basis, scaled, packed):
    total_gram = unpack_gram(second_core, value, other, packed)
    scaled[...] = total_gram / order
    row, column = indices(total_gram.shape[0])
    eye = row == column
    on_diag = jnp.where(eye, total_gram, 0.0)
    total = jnp.sum(jnp.sum(on_diag, axis=0, keepdims=True), axis=1, keepdims=True)
    half = jnp.where(eye, 1.5, 0.0)
    iterate = total_gram / total
    inverse = half - 0.5 * iterate
    parts = split(inverse)
    iterate = product(split(iterate), parts)
    for turn in range(1, NS_ITERS):
        held = parts
        moved = split(iterate)
        parts = split(half - 0.5 * product(held, moved))
        if turn < NS_ITERS - 1:
            iterate = product(moved, parts)
        inverse = product(parts, held)
        parts = split(inverse)
    scale = lax.sqrt(jnp.full_like(total, order)) / lax.sqrt(total)
    rows = basis.shape[0]
    basis[...] = product(split(payload[pl.ds(0, rows), :]), parts) * scale


def call(kernel, outs, operands, scratch=(), scalars=0, far=0, routes=0, aliases=None, limit=VMEM_LIMIT):
    shapes = tuple(jax.ShapeDtypeStruct(shape, dtype) for shape, dtype in outs)
    shapes += (jax.ShapeDtypeStruct((1,), jnp.int32),) * routes
    return pl.pallas_call(
        kernel,
        out_shape=shapes,
        in_specs=[SMEM] * scalars + [FAR] * far + [VMEM] * (len(operands) - scalars - far),
        out_specs=(VMEM,) * len(outs) + (SMEM,) * routes,
        scratch_shapes=[pltpu.VMEM(s, F32) if isinstance(s, tuple) else s for s in scratch],
        input_output_aliases=aliases or {},
        compiler_params=pltpu.CompilerParams(vmem_limit_bytes=limit),
    )(*operands)


def sum_over_devices(keep, send):
    value = keep + swap(send, lax.axis_size("gy"))
    for flips in ((1, 3, 2), (4, 20, 16), (32, 96, 64)):
        others = [swap(value, flip) for flip in flips]
        value = (value + others[0]) + (others[1] + others[2])
    return value, swap(value, lax.axis_size("gy"))


def on_device(subspace, diag_blocks, onsite, coupling, tile_rows, tile_cols, partner):
    colours = partner.shape[0]
    rows, states = subspace.shape
    size = coupling.shape[3]
    blocks = rows // size
    core = lax.axis_size("gy")
    wide, double = ((rows, states), F32), ((2 * rows, states), F32)
    parts = ((colours + 1, rows, rows), BF16)
    high, low, *state = call(
        functools.partial(prepare_kernel, core),
        (parts, parts, wide, double),
        (
            tile_rows, tile_cols, partner,
            diag_blocks, onsite.reshape(blocks, size), subspace, coupling[:, 0],
        ),
        ((blocks, blocks, size, size),),
        scalars=3,
        routes=2,
        limit=None,
    )

    def step(turn, state):
        acc, payload, place, flips_core = state
        got = exchange(place[0], flips_core[0], payload)
        return call(
            functools.partial(step_kernel, core),
            (wide, double),
            (turn.reshape(1), partner, high, low, got, subspace, acc, payload),
            (
                *(pltpu.VMEM((3, rows, rows), BF16),) * 2,
                (2 * rows, states),
                pltpu.SemaphoreType.DMA((3, 2)),
                pltpu.SemaphoreType.DMA((2,)),
            ),
            scalars=2,
            far=3,
            routes=2,
            aliases={6: 0, 7: 1},
        )

    _, payload, _, _ = lax.fori_loop(0, 2 * colours, step, tuple(state))
    second_core = (lax.axis_index("gx") & 1).reshape(1)
    packed = (states // 2 + PAD, states)
    share = ((packed[0] // 2, states), F32)
    keep, send = call(gram_kernel, (share, share), (second_core, payload), (packed,), scalars=1)
    return call(
        functools.partial(finish_kernel, float(rows * devices())),
        (wide, ((states, states), F32)),
        (second_core, *sum_over_devices(keep, send), payload),
        (packed,),
        scalars=1,
    )


def solution(mesh):
    placed = (
        P(AXES, None),
        P(AXES, None, None),
        P(AXES),
        P(None, AXES, None, None, None),
        P(None, AXES, None),
        P(None, AXES, None),
        P(),
    )
    return jax.shard_map(
        on_device,
        mesh=mesh,
        in_specs=placed,
        out_specs=(P(AXES, None), P()),
        check_vma=False,
    )
```

```python
import functools

import jax
import jax.numpy as jnp
from jax import lax
from jax.experimental import pallas as pl
from jax.experimental.pallas import tpu as pltpu
from jax.sharding import PartitionSpec as P

NS_ITERS = 12
AXES = ("gx", "gy")
VMEM = pl.BlockSpec(memory_space=pltpu.VMEM)
FAR = pl.BlockSpec(memory_space=pl.ANY)
SMEM = pl.BlockSpec(memory_space=pltpu.SMEM)
F32 = jnp.float32
BF16 = jnp.bfloat16
PAD = 16
VMEM_LIMIT = 28 << 20
NN = (((1,), (0,)), ((), ()))
TN = (((0,), (0,)), ((), ()))


def devices():
    return lax.axis_size("gx") * lax.axis_size("gy")


def swap(value, flip):
    return lax.ppermute(value, AXES, [(i, i ^ flip) for i in range(devices())])


def route(mask, core):
    above = lax.shift_right_logical(mask, jnp.int32(core.bit_length()))
    return (mask & (core - 1)) | (above * core), jnp.where((mask & core) != 0, 1, 0)


def exchange(place, flips_core, value):
    core = lax.axis_size("gy")
    keep = lambda kept: kept
    chips = [flip for flip in range(devices()) if not flip & core]
    movers = [functools.partial(swap, flip=flip) if flip else keep for flip in chips]
    value = lax.switch(place, movers, value)
    return lax.switch(flips_core, [keep, functools.partial(swap, flip=core)], value)


def split(value):
    high = value.astype(BF16)
    return high, (value - high.astype(F32)).astype(BF16)


def terms(high, low, right, dims=NN):
    dot = lambda a, b: lax.dot_general(a, b, dims, preferred_element_type=F32)
    return (dot(high, right[1]) + dot(low, right[0])) + dot(high, right[0])


def halves(size):
    return [pl.ds(start, size // 2) for start in (0, size // 2)]


def product(left, right, dims=NN):
    kept = 1 - dims[0][0][0]
    pieces = zip(*(jnp.split(part, 2, axis=kept) for part in left))
    return jnp.concatenate([terms(high, low, right, dims) for high, low in pieces], axis=0)


def indices(size):
    return tuple(lax.broadcasted_iota(jnp.int32, (size, size), axis) for axis in range(2))


def same_index(size):
    row, column = indices(size)
    return row == column


def prepare_kernel(
    core, tile_rows, tile_cols, partner, diag, onsite, own, tiles,
    high, low, acc, payload, place, flips_core, block,
):
    rows = own.shape[0]
    colours, count, size, _ = tiles.shape
    corners = range(rows // size)
    place[0], flips_core[0] = route(partner[0, 0], core)
    for c in range(colours):
        block[...] = jnp.zeros_like(block)
        for k in range(count):
            block[tile_rows[c, 0, k], tile_cols[c, 0, k]] += tiles[c, k]
        for r in corners:
            for s in corners:
                at = (pl.ds(r * size, size), pl.ds(s * size, size))
                high[(c, *at)], low[(c, *at)] = split(block[r, s])
    for r in corners:
        for s in corners:
            at = (pl.ds(r * size, size), pl.ds(s * size, size))
            value = diag[(0, *at)]
            if r == s:
                value += jnp.where(same_index(size), onsite[r : r + 1, :] - 2.0, 0.0)
            high[(colours, *at)], low[(colours, *at)] = split(value)
    value = own[...]
    parts = split(value)
    payload[pl.ds(0, rows), :] = value
    for half in halves(rows):
        acc[half, :] = terms(high[colours, half, :], low[colours, half, :], parts)
    for half in halves(rows):
        below = pl.ds(rows + half.start, half.size)
        payload[below, :] = terms(high[0, :, half], low[0, :, half], parts, TN)


def step_kernel(
    core, turn, partner, high, low, got, own, held_acc, held,
    acc, payload, place, flips_core, near_high, near_low, near, sems, near_sems,
):
    rows = own.shape[0]
    top, bottom = pl.ds(0, rows), pl.ds(rows, rows)
    colours = high.shape[0] - 1
    now = turn[0]
    colour, following = lax.rem(now, colours), lax.rem(now + 1, colours)
    last = colours * 2 - 1

    def fetch(index, slot):
        pairs = ((high, near_high), (low, near_low))
        return [
            pltpu.make_async_copy(far.at[index], close.at[slot], sems.at[slot, part])
            for part, (far, close) in enumerate(pairs)
        ]

    def wait(copies):
        for copy in copies:
            copy.wait()

    def below(half):
        return pl.ds(rows + half.start, half.size)

    def following_products(parts):
        for half in halves(rows):
            payload[below(half), :] = terms(near_high[0, :, half], near_low[0, :, half], parts, TN)

    backward, forward = fetch(following, 0), fetch(colour, 1)
    diagonal = fetch(colours, 2)
    arrived = [
        pltpu.make_async_copy(got.at[half], near.at[half], near_sems.at[part])
        for part, half in enumerate((top, bottom))
    ]
    for copy in backward + arrived[:1] + forward + arrived[1:]:
        copy.start()
    ends = colour == colours - 1

    @pl.when(now == colours - 1)
    def _():
        for copy in diagonal:
            copy.start()

    place[0], flips_core[0] = route(partner[following, 0], core)
    wait(backward)

    @pl.when(jnp.logical_not(ends))
    def _():
        value = held[top, :]
        payload[top, :] = value
        following_products(split(value))

    wait(arrived[:1] + forward + arrived[1:])
    mate = split(near[top, :])
    for half in halves(rows):
        kept = held_acc[half, :] + near[below(half), :]
        acc[half, :] = kept + terms(near_high[1, half, :], near_low[1, half, :], mate)

    @pl.when(now == colours - 1)
    def _():
        value = acc[...] * 0.25
        parts = split(value)
        payload[top, :] = value
        following_products(parts)
        wait(diagonal)
        for half in halves(rows):
            acc[half, :] = terms(near_high[2, half, :], near_low[2, half, :], parts)

    @pl.when(now == last)
    def _():
        payload[top, :] = acc[...] * 0.5 - own[...]


def gram_kernel(second_core, payload, keep, send, packed):
    states = payload.shape[1]
    half = states // 2
    parts = split(payload[pl.ds(0, payload.shape[0] // 2), :])
    gram = product(parts, parts, TN)
    row, column = indices(half)
    lower = gram[half:, half:]
    packed[pl.ds(0, half), :] = jnp.concatenate(
        [jnp.where(row <= column, gram[:half, :half], lower), gram[:half, half:]], axis=1
    )
    diagonal = jnp.sum(jnp.where(row == column, lower, 0.0), axis=0, keepdims=True)
    packed[pl.ds(half, PAD), :] = jnp.broadcast_to(
        jnp.concatenate([diagonal, diagonal], axis=1), (PAD, states)
    )
    share = packed.shape[0] // 2
    for own in range(2):

        @pl.when(second_core[0] == own)
        def _():
            keep[...] = packed[pl.ds(own * share, share), :]
            send[...] = packed[pl.ds((1 - own) * share, share), :]


def unpack_gram(second_core, value, other, packed):
    share = value.shape[0]
    for own in range(2):

        @pl.when(second_core[0] == own)
        def _():
            packed[pl.ds(own * share, share), :] = value[...]
            packed[pl.ds((1 - own) * share, share), :] = other[...]

    half = value.shape[1] // 2
    mixed, corner = packed[pl.ds(0, half), :half], packed[pl.ds(0, half), half:]
    turned = mixed.T
    row, column = indices(half)
    first = jnp.where(row <= column, mixed, turned)
    second = jnp.where(row > column, mixed, turned)
    second = jnp.where(row == column, packed[pl.ds(half, 1), :half], second)
    return jnp.concatenate(
        [jnp.concatenate([first, corner], axis=1), jnp.concatenate([corner.T, second], axis=1)],
        axis=0,
    )


def finish_kernel(order, second_core, value, other, payload, basis, scaled, packed):
    total_gram = unpack_gram(second_core, value, other, packed)
    scaled[...] = total_gram / order
    row, column = indices(total_gram.shape[0])
    eye = row == column
    on_diag = jnp.where(eye, total_gram, 0.0)
    total = jnp.sum(jnp.sum(on_diag, axis=0, keepdims=True), axis=1, keepdims=True)
    half = jnp.where(eye, 1.5, 0.0)
    iterate = total_gram / total
    inverse = half - 0.5 * iterate
    parts = split(inverse)
    iterate = product(split(iterate), parts)
    for turn in range(1, NS_ITERS):
        held = parts
        moved = split(iterate)
        parts = split(half - 0.5 * product(held, moved))
        if turn < NS_ITERS - 1:
            iterate = product(moved, parts)
        inverse = product(parts, held)
        parts = split(inverse)
    scale = lax.sqrt(jnp.full_like(total, order)) / lax.sqrt(total)
    rows = basis.shape[0]
    basis[...] = product(split(payload[pl.ds(0, rows), :]), parts) * scale


def call(kernel, outs, operands, scratch=(), scalars=0, far=0, routes=0, aliases=None, limit=VMEM_LIMIT):
    shapes = tuple(jax.ShapeDtypeStruct(shape, dtype) for shape, dtype in outs)
    shapes += (jax.ShapeDtypeStruct((1,), jnp.int32),) * routes
    return pl.pallas_call(
        kernel,
        out_shape=shapes,
        in_specs=[SMEM] * scalars + [FAR] * far + [VMEM] * (len(operands) - scalars - far),
        out_specs=(VMEM,) * len(outs) + (SMEM,) * routes,
        scratch_shapes=[pltpu.VMEM(s, F32) if isinstance(s, tuple) else s for s in scratch],
        input_output_aliases=aliases or {},
        compiler_params=pltpu.CompilerParams(vmem_limit_bytes=limit),
    )(*operands)


def sum_over_devices(keep, send):
    value = keep + swap(send, lax.axis_size("gy"))
    for flips in ((1, 3, 2), (4, 20, 16), (32, 96, 64)):
        others = [swap(value, flip) for flip in flips]
        value = (value + others[0]) + (others[1] + others[2])
    return value, swap(value, lax.axis_size("gy"))


def on_device(subspace, diag_blocks, onsite, coupling, tile_rows, tile_cols, partner):
    colours = partner.shape[0]
    rows, states = subspace.shape
    size = coupling.shape[3]
    blocks = rows // size
    core = lax.axis_size("gy")
    wide, double = ((rows, states), F32), ((2 * rows, states), F32)
    parts = ((colours + 1, rows, rows), BF16)
    high, low, *state = call(
        functools.partial(prepare_kernel, core),
        (parts, parts, wide, double),
        (
            tile_rows, tile_cols, partner,
            diag_blocks, onsite.reshape(blocks, size), subspace, coupling[:, 0],
        ),
        ((blocks, blocks, size, size),),
        scalars=3,
        routes=2,
        limit=None,
    )

    def step(turn, state):
        acc, payload, place, flips_core = state
        got = exchange(place[0], flips_core[0], payload)
        return call(
            functools.partial(step_kernel, core),
            (wide, double),
            (turn.reshape(1), partner, high, low, got, subspace, acc, payload),
            (
                *(pltpu.VMEM((3, rows, rows), BF16),) * 2,
                (2 * rows, states),
                pltpu.SemaphoreType.DMA((3, 2)),
                pltpu.SemaphoreType.DMA((2,)),
            ),
            scalars=2,
            far=3,
            routes=2,
            aliases={6: 0, 7: 1},
        )

    _, payload, _, _ = lax.fori_loop(0, 2 * colours, step, tuple(state))
    second_core = (lax.axis_index("gx") & 1).reshape(1)
    packed = (states // 2 + PAD, states)
    share = ((packed[0] // 2, states), F32)
    keep, send = call(gram_kernel, (share, share), (second_core, payload), (packed,), scalars=1)
    return call(
        functools.partial(finish_kernel, float(rows * devices())),
        (wide, ((states, states), F32)),
        (second_core, *sum_over_devices(keep, send), payload),
        (packed,),
        scalars=1,
    )


def solution(mesh):
    placed = (
        P(AXES, None),
        P(AXES, None, None),
        P(AXES),
        P(None, AXES, None, None, None),
        P(None, AXES, None),
        P(None, AXES, None),
        P(),
    )
    return jax.shard_map(
        on_device,
        mesh=mesh,
        in_specs=placed,
        out_specs=(P(AXES, None), P()),
        check_vma=False,
    )
```

```python
import functools

import jax
import jax.numpy as jnp
from jax import lax
from jax.experimental import pallas as pl
from jax.experimental.pallas import tpu as pltpu
from jax.sharding import PartitionSpec as P

NS_ITERS = 12
AXES = ("gx", "gy")
VMEM = pl.BlockSpec(memory_space=pltpu.VMEM)
FAR = pl.BlockSpec(memory_space=pl.ANY)
SMEM = pl.BlockSpec(memory_space=pltpu.SMEM)
F32 = jnp.float32
BF16 = jnp.bfloat16
PAD = 16
VMEM_LIMIT = 28 << 20
NN = (((1,), (0,)), ((), ()))
TN = (((0,), (0,)), ((), ()))


def devices():
    return lax.axis_size("gx") * lax.axis_size("gy")


def swap(value, flip):
    return lax.ppermute(value, AXES, [(i, i ^ flip) for i in range(devices())])


def route(mask, core):
    above = lax.shift_right_logical(mask, jnp.int32(core.bit_length()))
    return (mask & (core - 1)) | (above * core), jnp.where((mask & core) != 0, 1, 0)


def exchange(place, flips_core, value):
    core = lax.axis_size("gy")
    keep = lambda kept: kept
    chips = [flip for flip in range(devices()) if not flip & core]
    movers = [functools.partial(swap, flip=flip) if flip else keep for flip in chips]
    value = lax.switch(place, movers, value)
    return lax.switch(flips_core, [keep, functools.partial(swap, flip=core)], value)


def split(value):
    high = value.astype(BF16)
    return high, (value - high.astype(F32)).astype(BF16)


def terms(high, low, right, dims=NN):
    dot = lambda a, b: lax.dot_general(a, b, dims, preferred_element_type=F32)
    return (dot(high, right[1]) + dot(low, right[0])) + dot(high, right[0])


def halves(size):
    return [pl.ds(start, size // 2) for start in (0, size // 2)]


def product(left, right, dims=NN):
    kept = 1 - dims[0][0][0]
    pieces = zip(*(jnp.split(part, 2, axis=kept) for part in left))
    return jnp.concatenate([terms(high, low, right, dims) for high, low in pieces], axis=0)


def indices(size):
    return tuple(lax.broadcasted_iota(jnp.int32, (size, size), axis) for axis in range(2))


def same_index(size):
    row, column = indices(size)
    return row == column


def prepare_kernel(
    core, tile_rows, tile_cols, partner, far_diag, far_own, far_tiles, onsite,
    high, low, acc, payload, place, flips_core, block, diag, own, tiles, sems,
):
    rows = own.shape[0]
    colours, count, size, _ = tiles.shape
    pairs = [(far_tiles.at[c], tiles.at[c]) for c in range(colours)]
    pairs += [(far_own, own), (far_diag.at[0], diag)]
    loads = [pltpu.make_async_copy(*pair, sems.at[i]) for i, pair in enumerate(pairs)]
    for load in loads:
        load.start()
    corners = range(rows // size)
    place[0], flips_core[0] = route(partner[0, 0], core)
    for c in range(colours):
        block[...] = jnp.zeros_like(block)
        loads[c].wait()
        for k in range(count):
            block[tile_rows[c, 0, k], tile_cols[c, 0, k]] += tiles[c, k]
        for r in corners:
            for s in corners:
                at = (pl.ds(r * size, size), pl.ds(s * size, size))
                high[(c, *at)], low[(c, *at)] = split(block[r, s])
    loads[colours].wait()
    loads[colours + 1].wait()
    for r in corners:
        for s in corners:
            at = (pl.ds(r * size, size), pl.ds(s * size, size))
            value = diag[at]
            if r == s:
                value += jnp.where(same_index(size), onsite[r : r + 1, :] - 2.0, 0.0)
            high[(colours, *at)], low[(colours, *at)] = split(value)
    value = own[...]
    parts = split(value)
    payload[pl.ds(0, rows), :] = value
    for half in halves(rows):
        acc[half, :] = terms(high[colours, half, :], low[colours, half, :], parts)
    for half in halves(rows):
        below = pl.ds(rows + half.start, half.size)
        payload[below, :] = terms(high[0, :, half], low[0, :, half], parts, TN)


def step_kernel(
    core, turn, partner, high, low, got, own, held_acc, held,
    acc, payload, place, flips_core, near_high, near_low, near, sems, near_sems,
):
    rows = own.shape[0]
    top, bottom = pl.ds(0, rows), pl.ds(rows, rows)
    colours = high.shape[0] - 1
    now = turn[0]
    colour, following = lax.rem(now, colours), lax.rem(now + 1, colours)
    last = colours * 2 - 1

    def fetch(index, slot):
        pairs = ((high, near_high), (low, near_low))
        return [
            pltpu.make_async_copy(far.at[index], close.at[slot], sems.at[slot, part])
            for part, (far, close) in enumerate(pairs)
        ]

    def wait(copies):
        for copy in copies:
            copy.wait()

    def below(half):
        return pl.ds(rows + half.start, half.size)

    def following_products(parts):
        for half in halves(rows):
            payload[below(half), :] = terms(near_high[0, :, half], near_low[0, :, half], parts, TN)

    backward, forward = fetch(following, 0), fetch(colour, 1)
    diagonal = fetch(colours, 2)
    arrived = [
        pltpu.make_async_copy(got.at[half], near.at[half], near_sems.at[part])
        for part, half in enumerate((top, bottom))
    ]
    for copy in backward + arrived[:1] + forward + arrived[1:]:
        copy.start()
    ends = colour == colours - 1

    @pl.when(now == colours - 1)
    def _():
        for copy in diagonal:
            copy.start()

    place[0], flips_core[0] = route(partner[following, 0], core)
    wait(backward)

    @pl.when(jnp.logical_not(ends))
    def _():
        value = held[top, :]
        payload[top, :] = value
        following_products(split(value))

    wait(arrived[:1] + forward + arrived[1:])
    mate = split(near[top, :])
    for half in halves(rows):
        kept = held_acc[half, :] + near[below(half), :]
        acc[half, :] = kept + terms(near_high[1, half, :], near_low[1, half, :], mate)

    @pl.when(now == colours - 1)
    def _():
        value = acc[...] * 0.25
        parts = split(value)
        payload[top, :] = value
        following_products(parts)
        wait(diagonal)
        for half in halves(rows):
            acc[half, :] = terms(near_high[2, half, :], near_low[2, half, :], parts)

    @pl.when(now == last)
    def _():
        payload[top, :] = acc[...] * 0.5 - own[...]


def gram_kernel(second_core, payload, keep, send, packed):
    states = payload.shape[1]
    half = states // 2
    parts = split(payload[pl.ds(0, payload.shape[0] // 2), :])
    gram = product(parts, parts, TN)
    row, column = indices(half)
    lower = gram[half:, half:]
    packed[pl.ds(0, half), :] = jnp.concatenate(
        [jnp.where(row <= column, gram[:half, :half], lower), gram[:half, half:]], axis=1
    )
    diagonal = jnp.sum(jnp.where(row == column, lower, 0.0), axis=0, keepdims=True)
    packed[pl.ds(half, PAD), :] = jnp.broadcast_to(
        jnp.concatenate([diagonal, diagonal], axis=1), (PAD, states)
    )
    share = packed.shape[0] // 2
    for own in range(2):

        @pl.when(second_core[0] == own)
        def _():
            keep[...] = packed[pl.ds(own * share, share), :]
            send[...] = packed[pl.ds((1 - own) * share, share), :]


def unpack_gram(second_core, value, other, packed):
    share = value.shape[0]
    for own in range(2):

        @pl.when(second_core[0] == own)
        def _():
            packed[pl.ds(own * share, share), :] = value[...]
            packed[pl.ds((1 - own) * share, share), :] = other[...]

    half = value.shape[1] // 2
    mixed, corner = packed[pl.ds(0, half), :half], packed[pl.ds(0, half), half:]
    turned = mixed.T
    row, column = indices(half)
    first = jnp.where(row <= column, mixed, turned)
    second = jnp.where(row > column, mixed, turned)
    second = jnp.where(row == column, packed[pl.ds(half, 1), :half], second)
    return jnp.concatenate(
        [jnp.concatenate([first, corner], axis=1), jnp.concatenate([corner.T, second], axis=1)],
        axis=0,
    )


def finish_kernel(order, second_core, value, other, payload, basis, scaled, packed):
    total_gram = unpack_gram(second_core, value, other, packed)
    scaled[...] = total_gram / order
    row, column = indices(total_gram.shape[0])
    eye = row == column
    on_diag = jnp.where(eye, total_gram, 0.0)
    total = jnp.sum(jnp.sum(on_diag, axis=0, keepdims=True), axis=1, keepdims=True)
    half = jnp.where(eye, 1.5, 0.0)
    iterate = total_gram / total
    inverse = half - 0.5 * iterate
    parts = split(inverse)
    iterate = product(split(iterate), parts)
    for turn in range(1, NS_ITERS):
        held = parts
        moved = split(iterate)
        parts = split(half - 0.5 * product(held, moved))
        if turn < NS_ITERS - 1:
            iterate = product(moved, parts)
        inverse = product(parts, held)
        parts = split(inverse)
    scale = lax.sqrt(jnp.full_like(total, order)) / lax.sqrt(total)
    rows = basis.shape[0]
    basis[...] = product(split(payload[pl.ds(0, rows), :]), parts) * scale


def call(kernel, outs, operands, scratch=(), scalars=0, far=0, routes=0, aliases=None, limit=VMEM_LIMIT):
    shapes = tuple(jax.ShapeDtypeStruct(shape, dtype) for shape, dtype in outs)
    shapes += (jax.ShapeDtypeStruct((1,), jnp.int32),) * routes
    return pl.pallas_call(
        kernel,
        out_shape=shapes,
        in_specs=[SMEM] * scalars + [FAR] * far + [VMEM] * (len(operands) - scalars - far),
        out_specs=(VMEM,) * len(outs) + (SMEM,) * routes,
        scratch_shapes=[pltpu.VMEM(s, F32) if isinstance(s, tuple) else s for s in scratch],
        input_output_aliases=aliases or {},
        compiler_params=pltpu.CompilerParams(vmem_limit_bytes=limit),
    )(*operands)


def sum_over_devices(keep, send):
    value = keep + swap(send, lax.axis_size("gy"))
    for flips in ((1, 3, 2), (4, 20, 16), (32, 96, 64)):
        others = [swap(value, flip) for flip in flips]
        value = (value + others[0]) + (others[1] + others[2])
    return value, swap(value, lax.axis_size("gy"))


def on_device(subspace, diag_blocks, onsite, coupling, tile_rows, tile_cols, partner):
    colours = partner.shape[0]
    rows, states = subspace.shape
    size = coupling.shape[3]
    blocks = rows // size
    core = lax.axis_size("gy")
    wide, double = ((rows, states), F32), ((2 * rows, states), F32)
    parts = ((colours + 1, rows, rows), BF16)
    high, low, *state = call(
        functools.partial(prepare_kernel, core),
        (parts, parts, wide, double),
        (
            tile_rows, tile_cols, partner,
            diag_blocks, subspace, coupling[:, 0], onsite.reshape(blocks, size),
        ),
        (
            (blocks, blocks, size, size),
            (rows, rows),
            (rows, states),
            (colours, *coupling.shape[2:]),
            pltpu.SemaphoreType.DMA((colours + 2,)),
        ),
        scalars=3,
        far=3,
        routes=2,
        limit=None,
    )

    def step(turn, state):
        acc, payload, place, flips_core = state
        got = exchange(place[0], flips_core[0], payload)
        return call(
            functools.partial(step_kernel, core),
            (wide, double),
            (turn.reshape(1), partner, high, low, got, subspace, acc, payload),
            (
                *(pltpu.VMEM((3, rows, rows), BF16),) * 2,
                (2 * rows, states),
                pltpu.SemaphoreType.DMA((3, 2)),
                pltpu.SemaphoreType.DMA((2,)),
            ),
            scalars=2,
            far=3,
            routes=2,
            aliases={6: 0, 7: 1},
        )

    _, payload, _, _ = lax.fori_loop(0, 2 * colours, step, tuple(state))
    second_core = (lax.axis_index("gx") & 1).reshape(1)
    packed = (states // 2 + PAD, states)
    share = ((packed[0] // 2, states), F32)
    keep, send = call(gram_kernel, (share, share), (second_core, payload), (packed,), scalars=1)
    return call(
        functools.partial(finish_kernel, float(rows * devices())),
        (wide, ((states, states), F32)),
        (second_core, *sum_over_devices(keep, send), payload),
        (packed,),
        scalars=1,
    )


def solution(mesh):
    placed = (
        P(AXES, None),
        P(AXES, None, None),
        P(AXES),
        P(None, AXES, None, None, None),
        P(None, AXES, None),
        P(None, AXES, None),
        P(),
    )
    return jax.shard_map(
        on_device,
        mesh=mesh,
        in_specs=placed,
        out_specs=(P(AXES, None), P()),
        check_vma=False,
    )
```

```python
import functools

import jax
import jax.numpy as jnp
from jax import lax
from jax.experimental import pallas as pl
from jax.experimental.pallas import tpu as pltpu
from jax.sharding import PartitionSpec as P

NS_ITERS = 12
AXES = ("gx", "gy")
VMEM = pl.BlockSpec(memory_space=pltpu.VMEM)
FAR = pl.BlockSpec(memory_space=pl.ANY)
SMEM = pl.BlockSpec(memory_space=pltpu.SMEM)
F32 = jnp.float32
BF16 = jnp.bfloat16
PAD = 16
VMEM_LIMIT = 28 << 20
NN = (((1,), (0,)), ((), ()))
TN = (((0,), (0,)), ((), ()))


def devices():
    return lax.axis_size("gx") * lax.axis_size("gy")


def swap(value, flip):
    return lax.ppermute(value, AXES, [(i, i ^ flip) for i in range(devices())])


def route(mask, core):
    above = lax.shift_right_logical(mask, jnp.int32(core.bit_length()))
    return (mask & (core - 1)) | (above * core), jnp.where((mask & core) != 0, 1, 0)


def exchange(place, flips_core, value):
    core = lax.axis_size("gy")
    keep = lambda kept: kept
    chips = [flip for flip in range(devices()) if not flip & core]
    movers = [functools.partial(swap, flip=flip) if flip else keep for flip in chips]
    value = lax.switch(place, movers, value)
    return lax.switch(flips_core, [keep, functools.partial(swap, flip=core)], value)


def split(value):
    high = value.astype(BF16)
    return high, (value - high.astype(F32)).astype(BF16)


def terms(high, low, right, dims=NN):
    dot = lambda a, b: lax.dot_general(a, b, dims, preferred_element_type=F32)
    return (dot(high, right[1]) + dot(low, right[0])) + dot(high, right[0])


def halves(size):
    return [pl.ds(start, size // 2) for start in (0, size // 2)]


def product(left, right, dims=NN):
    kept = 1 - dims[0][0][0]
    pieces = zip(*(jnp.split(part, 2, axis=kept) for part in left))
    return jnp.concatenate([terms(high, low, right, dims) for high, low in pieces], axis=0)


def indices(size):
    return tuple(lax.broadcasted_iota(jnp.int32, (size, size), axis) for axis in range(2))


def same_index(size):
    row, column = indices(size)
    return row == column


def prepare_kernel(
    core, tile_rows, tile_cols, partner, far_diag, far_own, far_tiles, onsite,
    high, low, acc, payload, place, flips_core, block, diag, own, tiles, sems,
):
    rows = own.shape[0]
    colours, count, size, _ = tiles.shape
    pairs = [(far_tiles.at[c], tiles.at[c]) for c in range(colours)]
    pairs += [(far_own, own), (far_diag.at[0], diag)]
    loads = [pltpu.make_async_copy(*pair, sems.at[i]) for i, pair in enumerate(pairs)]
    for load in loads:
        load.start()
    corners = range(rows // size)
    place[0], flips_core[0] = route(partner[0, 0], core)
    for c in range(colours):
        block[...] = jnp.zeros_like(block)
        loads[c].wait()
        for k in range(count):
            block[tile_rows[c, 0, k], tile_cols[c, 0, k]] += tiles[c, k]
        for r in corners:
            for s in corners:
                at = (pl.ds(r * size, size), pl.ds(s * size, size))
                high[(c, *at)], low[(c, *at)] = split(block[r, s])
    loads[colours].wait()
    loads[colours + 1].wait()
    for r in corners:
        for s in corners:
            at = (pl.ds(r * size, size), pl.ds(s * size, size))
            value = diag[at]
            if r == s:
                value += jnp.where(same_index(size), onsite[r : r + 1, :] - 2.0, 0.0)
            high[(colours, *at)], low[(colours, *at)] = split(value)
    value = own[...]
    parts = split(value)
    payload[pl.ds(0, rows), :] = value
    for half in halves(rows):
        acc[half, :] = terms(high[colours, half, :], low[colours, half, :], parts)
    for half in halves(rows):
        below = pl.ds(rows + half.start, half.size)
        payload[below, :] = terms(high[0, :, half], low[0, :, half], parts, TN)


def step_kernel(
    core, turn, partner, high, low, got, own, held_acc, held,
    acc, payload, place, flips_core, near_high, near_low, near, sems, near_sems,
):
    rows = own.shape[0]
    top, bottom = pl.ds(0, rows), pl.ds(rows, rows)
    colours = high.shape[0] - 1
    now = turn[0]
    colour, following = lax.rem(now, colours), lax.rem(now + 1, colours)
    last = colours * 2 - 1

    def fetch(index, slot):
        pairs = ((high, near_high), (low, near_low))
        return [
            pltpu.make_async_copy(far.at[index], close.at[slot], sems.at[slot, part])
            for part, (far, close) in enumerate(pairs)
        ]

    def wait(copies):
        for copy in copies:
            copy.wait()

    def below(half):
        return pl.ds(rows + half.start, half.size)

    def following_products(parts):
        for half in halves(rows):
            payload[below(half), :] = terms(near_high[0, :, half], near_low[0, :, half], parts, TN)

    backward, forward = fetch(following, 0), fetch(colour, 1)
    diagonal = fetch(colours, 2)
    arrived = [
        pltpu.make_async_copy(got.at[half], near.at[half], near_sems.at[part])
        for part, half in enumerate((top, bottom))
    ]
    ends = colour == colours - 1

    def start(copies):
        for copy in copies:
            copy.start()

    @pl.when(jnp.logical_not(ends))
    def _():
        start(backward)

    start(arrived[:1] + forward + arrived[1:])

    @pl.when(now == colours - 1)
    def _():
        start(backward + diagonal)

    place[0], flips_core[0] = route(partner[following, 0], core)
    @pl.when(jnp.logical_not(ends))
    def _():
        wait(backward)
        value = held[top, :]
        payload[top, :] = value
        following_products(split(value))

    wait(arrived[:1] + forward + arrived[1:])
    mate = split(near[top, :])
    for half in halves(rows):
        kept = held_acc[half, :] + near[below(half), :]
        acc[half, :] = kept + terms(near_high[1, half, :], near_low[1, half, :], mate)

    @pl.when(now == colours - 1)
    def _():
        value = acc[...] * 0.25
        parts = split(value)
        payload[top, :] = value
        wait(backward)
        following_products(parts)
        wait(diagonal)
        for half in halves(rows):
            acc[half, :] = terms(near_high[2, half, :], near_low[2, half, :], parts)

    @pl.when(now == last)
    def _():
        payload[top, :] = acc[...] * 0.5 - own[...]


def gram_kernel(second_core, payload, keep, send, packed):
    states = payload.shape[1]
    half = states // 2
    parts = split(payload[pl.ds(0, payload.shape[0] // 2), :])
    gram = product(parts, parts, TN)
    row, column = indices(half)
    lower = gram[half:, half:]
    packed[pl.ds(0, half), :] = jnp.concatenate(
        [jnp.where(row <= column, gram[:half, :half], lower), gram[:half, half:]], axis=1
    )
    diagonal = jnp.sum(jnp.where(row == column, lower, 0.0), axis=0, keepdims=True)
    packed[pl.ds(half, PAD), :] = jnp.broadcast_to(
        jnp.concatenate([diagonal, diagonal], axis=1), (PAD, states)
    )
    share = packed.shape[0] // 2
    for own in range(2):

        @pl.when(second_core[0] == own)
        def _():
            keep[...] = packed[pl.ds(own * share, share), :]
            send[...] = packed[pl.ds((1 - own) * share, share), :]


def unpack_gram(second_core, value, other, packed):
    share = value.shape[0]
    for own in range(2):

        @pl.when(second_core[0] == own)
        def _():
            packed[pl.ds(own * share, share), :] = value[...]
            packed[pl.ds((1 - own) * share, share), :] = other[...]

    half = value.shape[1] // 2
    mixed, corner = packed[pl.ds(0, half), :half], packed[pl.ds(0, half), half:]
    turned = mixed.T
    row, column = indices(half)
    first = jnp.where(row <= column, mixed, turned)
    second = jnp.where(row > column, mixed, turned)
    second = jnp.where(row == column, packed[pl.ds(half, 1), :half], second)
    return jnp.concatenate(
        [jnp.concatenate([first, corner], axis=1), jnp.concatenate([corner.T, second], axis=1)],
        axis=0,
    )


def finish_kernel(order, second_core, value, other, payload, basis, scaled, packed):
    total_gram = unpack_gram(second_core, value, other, packed)
    scaled[...] = total_gram / order
    row, column = indices(total_gram.shape[0])
    eye = row == column
    on_diag = jnp.where(eye, total_gram, 0.0)
    total = jnp.sum(jnp.sum(on_diag, axis=0, keepdims=True), axis=1, keepdims=True)
    half = jnp.where(eye, 1.5, 0.0)
    iterate = total_gram / total
    inverse = half - 0.5 * iterate
    parts = split(inverse)
    iterate = product(split(iterate), parts)
    for turn in range(1, NS_ITERS):
        held = parts
        moved = split(iterate)
        parts = split(half - 0.5 * product(held, moved))
        if turn < NS_ITERS - 1:
            iterate = product(moved, parts)
        inverse = product(parts, held)
        parts = split(inverse)
    scale = lax.sqrt(jnp.full_like(total, order)) / lax.sqrt(total)
    rows = basis.shape[0]
    basis[...] = product(split(payload[pl.ds(0, rows), :]), parts) * scale


def call(kernel, outs, operands, scratch=(), scalars=0, far=0, routes=0, aliases=None, limit=VMEM_LIMIT):
    shapes = tuple(jax.ShapeDtypeStruct(shape, dtype) for shape, dtype in outs)
    shapes += (jax.ShapeDtypeStruct((1,), jnp.int32),) * routes
    return pl.pallas_call(
        kernel,
        out_shape=shapes,
        in_specs=[SMEM] * scalars + [FAR] * far + [VMEM] * (len(operands) - scalars - far),
        out_specs=(VMEM,) * len(outs) + (SMEM,) * routes,
        scratch_shapes=[pltpu.VMEM(s, F32) if isinstance(s, tuple) else s for s in scratch],
        input_output_aliases=aliases or {},
        compiler_params=pltpu.CompilerParams(vmem_limit_bytes=limit),
    )(*operands)


def sum_over_devices(keep, send):
    value = keep + swap(send, lax.axis_size("gy"))
    for flips in ((1, 3, 2), (4, 20, 16), (32, 96, 64)):
        others = [swap(value, flip) for flip in flips]
        value = (value + others[0]) + (others[1] + others[2])
    return value, swap(value, lax.axis_size("gy"))


def on_device(subspace, diag_blocks, onsite, coupling, tile_rows, tile_cols, partner):
    colours = partner.shape[0]
    rows, states = subspace.shape
    size = coupling.shape[3]
    blocks = rows // size
    core = lax.axis_size("gy")
    wide, double = ((rows, states), F32), ((2 * rows, states), F32)
    parts = ((colours + 1, rows, rows), BF16)
    high, low, *state = call(
        functools.partial(prepare_kernel, core),
        (parts, parts, wide, double),
        (
            tile_rows, tile_cols, partner,
            diag_blocks, subspace, coupling[:, 0], onsite.reshape(blocks, size),
        ),
        (
            (blocks, blocks, size, size),
            (rows, rows),
            (rows, states),
            (colours, *coupling.shape[2:]),
            pltpu.SemaphoreType.DMA((colours + 2,)),
        ),
        scalars=3,
        far=3,
        routes=2,
        limit=None,
    )

    def step(turn, state):
        acc, payload, place, flips_core = state
        got = exchange(place[0], flips_core[0], payload)
        return call(
            functools.partial(step_kernel, core),
            (wide, double),
            (turn.reshape(1), partner, high, low, got, subspace, acc, payload),
            (
                *(pltpu.VMEM((3, rows, rows), BF16),) * 2,
                (2 * rows, states),
                pltpu.SemaphoreType.DMA((3, 2)),
                pltpu.SemaphoreType.DMA((2,)),
            ),
            scalars=2,
            far=3,
            routes=2,
            aliases={6: 0, 7: 1},
        )

    _, payload, _, _ = lax.fori_loop(0, 2 * colours, step, tuple(state))
    second_core = (lax.axis_index("gx") & 1).reshape(1)
    packed = (states // 2 + PAD, states)
    share = ((packed[0] // 2, states), F32)
    keep, send = call(gram_kernel, (share, share), (second_core, payload), (packed,), scalars=1)
    return call(
        functools.partial(finish_kernel, float(rows * devices())),
        (wide, ((states, states), F32)),
        (second_core, *sum_over_devices(keep, send), payload),
        (packed,),
        scalars=1,
    )


def solution(mesh):
    placed = (
        P(AXES, None),
        P(AXES, None, None),
        P(AXES),
        P(None, AXES, None, None, None),
        P(None, AXES, None),
        P(None, AXES, None),
        P(),
    )
    return jax.shard_map(
        on_device,
        mesh=mesh,
        in_specs=placed,
        out_specs=(P(AXES, None), P()),
        check_vma=False,
    )
```
